32 devices in a mesh: seq: 8 (over z, y), head: 4 (over x, core).
Axes of the slice: x: 2, y: 2, z: 4, core: 2. Of those that a mesh axis runs over, the one named last changes fastest.
Arguments:
- query_rows: bfloat16 [4096, 4096], P('seq', 'head'), may hold values from -6 to 6
- key_rows: bfloat16 [4096, 4096], P('seq', 'head'), may hold values from -2 to 2
- value_rows: bfloat16 [4096, 4096], P('seq', 'head'), may hold values from -6 to 6
- key_gain: float32 [32], P('head'), may hold values from 0.9 to 1.85, as said below
- regularizer: float32 [32], P('head'), may hold values from 0.5 to 4
Outputs:
- readout: bfloat16 [4096, 4096], P('seq', 'head')
The draws below stay inside these ranges and needn't reach their ends.
Inputs may be any that keep to these rules, and one draw needn't show every extreme that they name: `key_gain`: one positive gain for each head.
All inputs are finite; a program needn't handle non-finite values.
Results may differ from the reference program's by a relative error of at most 0.006.
Values sent between devices are 32-bit elements; how exact they have to be, the bound alone decides.
A program may use at most 192 MiB of HBM per device.

```python
import math
import jax
import jax.numpy as jnp
from jax import lax

DH = 128
HEADS = 32
TOK_DEV = 512
NS_STEPS = 8
REFINE = 2
SEQ = 4096


def draw_key_gain(key, part):
    position = jnp.arange(HEADS, dtype=jnp.float32) / (HEADS - 1)
    return jnp.exp(0.5 * position + jax.random.uniform(key, (HEADS,), jnp.float32, -0.1, 0.1))


def draw_key_rows(key, part):
    column_key = jax.random.fold_in(key, 11)
    entry_key = jax.random.fold_in(key, 12)
    width = HEADS * DH
    amplitude = jnp.exp(jax.random.uniform(column_key, (width,), jnp.float32, math.log(0.3), math.log(2.4)))
    entries = jax.random.truncated_normal(entry_key, -4.0, 4.0, (SEQ, width), jnp.float32)
    return (entries * amplitude[None, :] / math.sqrt(DH)).astype(jnp.bfloat16)


def steps_of(key, dims, shards, low, largest):
    level = 1.0
    for axis_at, blocks in shards:
        heights = jax.random.uniform(jax.random.fold_in(jax.random.fold_in(key, 6), axis_at), (blocks,), jnp.float32, low / len(shards), largest / len(shards))
        level = level * jnp.repeat(jnp.exp(heights), dims[axis_at] // blocks).reshape((-1,) + (1,) * (len(dims) - 1 - axis_at))
    return level


def gaussian(stream_key, extent, scale, most, cuts=(), held_as=jnp.bfloat16):
    gain = steps_of(stream_key, extent, cuts, -0.22, 0.18) if cuts else 1.0
    values = jax.random.normal(stream_key, extent, jnp.float32) * scale * gain
    return jnp.minimum(jnp.maximum(values, -most), most).astype(held_as)


def setup_inputs(seed: int = 0) -> dict:
    seeds = jax.random.split(jax.random.key(seed), 6)
    return {
        "query_rows": gaussian(seeds[0], (SEQ, HEADS * DH), 1.0, 6.0, ((0, 8), (1, 4))),
        "key_rows": draw_key_rows(jax.random.fold_in(seeds[5], 71), 0),
        "value_rows": gaussian(seeds[2], (SEQ, HEADS * DH), 1.0, 6.0, ((0, 8), (1, 4))),
        "key_gain": draw_key_gain(jax.random.fold_in(seeds[5], 71), 0),
        "regularizer": jnp.clip(jnp.exp(math.log(4.0) - 2.0794415 * jax.random.uniform(seeds[4], (HEADS,), jnp.float32) ** steps_of(seeds[4], (HEADS,), ((0, 4),), -0.2, 0.2)), 0.5, 4.0),
    }


highest = lax.Precision.HIGHEST

def contract_rows(left, right):
    return lax.dot_general(left, right, (((1,), (1,)), ((), ())), preferred_element_type=jnp.float32)

def invert_scaled(end_matrix, spectral_bound):
    identity = jnp.eye(end_matrix.shape[-1], dtype=jnp.float32)
    approx = identity[None, :, :] / spectral_bound[:, None, None]
    for iteration in range(NS_STEPS):
        product = jnp.einsum('hij,hjk->hik', end_matrix, approx, precision=highest)
        approx = jnp.einsum('hij,hjk->hik', approx, 2.0 * identity - product, precision=highest)
    return approx

def solve_head(operands):
    query_head, key_head, value_head, base_matrix, precond, cross_matrix = operands
    length = query_head.shape[0]
    causal = jnp.arange(length)[:, None] >= jnp.arange(length)[None, :]
    query_float = query_head.astype(jnp.float32)
    solution = jnp.dot(query_float, precond, precision=highest)
    for repeat in range(REFINE):
        scores = jnp.where(causal, contract_rows(solution.astype(jnp.bfloat16), key_head), 0.0).astype(jnp.bfloat16)
        in_block = jnp.dot(scores, key_head, preferred_element_type=jnp.float32)
        residual = query_float - jnp.dot(solution, base_matrix, precision=highest) - in_block
        solution = solution + jnp.dot(residual, precond, precision=highest)
    scores = jnp.where(causal, contract_rows(solution.astype(jnp.bfloat16), key_head), 0.0).astype(jnp.bfloat16)
    total = jnp.dot(solution, cross_matrix, precision=highest) + jnp.dot(scores, value_head, preferred_element_type=jnp.float32)
    return total.astype(jnp.bfloat16)

def reference(query_rows, key_rows, value_rows, key_gain, regularizer):
    block_count = query_rows.shape[0] // TOK_DEV
    split_shape = (block_count, TOK_DEV, HEADS, DH)
    identity = jnp.eye(DH, dtype=jnp.float32)

    def block_step(carry, operands):
        prior_gram, prior_cross = carry
        query_block, key_block, value_block = operands
        scaled = (key_block.astype(jnp.float32) * key_gain[None, :, None]).astype(jnp.bfloat16)
        scaled_float = scaled.astype(jnp.float32)
        gram_block = jnp.einsum('thd,the->hde', scaled_float, scaled_float, precision=highest)
        cross_block = jnp.einsum('thd,the->hde', scaled_float, value_block.astype(jnp.float32), precision=highest)
        base_matrix = regularizer[:, None, None] * identity + prior_gram
        end_matrix = base_matrix + gram_block
        spectral_bound = jnp.sqrt(lax.optimization_barrier(jnp.sum(end_matrix * end_matrix, axis=(1, 2))))
        precond = invert_scaled(end_matrix, spectral_bound)
        readout = lax.map(solve_head, (jnp.transpose(query_block, (1, 0, 2)), jnp.transpose(scaled, (1, 0, 2)), jnp.transpose(value_block, (1, 0, 2)), base_matrix, precond, prior_cross))
        merged = jnp.transpose(readout, (1, 0, 2)).reshape(TOK_DEV, HEADS * DH)
        return ((prior_gram + gram_block, prior_cross + cross_block), merged)
    empty_state = jnp.zeros((HEADS, DH, DH), jnp.float32)
    final_carry, outputs = lax.scan(block_step, (empty_state, empty_state), (query_rows.reshape(split_shape), key_rows.reshape(split_shape), value_rows.reshape(split_shape)))
    return outputs.reshape(block_count * TOK_DEV, HEADS * DH)
```

```python
import functools

import jax
import jax.numpy as jnp
from jax import lax
from jax.experimental import pallas as pl
from jax.experimental.pallas import tpu as pltpu
from jax.sharding import PartitionSpec as P

NS_STEPS = 8
REFINE = 2
LANES = 2
F32 = jnp.float32
BF16 = jnp.bfloat16
MESH = pl.DeviceIdType.MESH


def mm(left, right):
    return lax.dot_general(left, right, (((1,), (0,)), ((), ())), preferred_element_type=F32)


def mm_nt(left, right):
    return lax.dot_general(left, right, (((1,), (1,)), ((), ())), preferred_element_type=F32)


def mm_tn(left, right):
    return lax.dot_general(left, right, (((0,), (0,)), ((), ())), preferred_element_type=F32)


def halves(value):
    high = value.astype(BF16)
    low = (value - high.astype(F32)).astype(BF16)
    return jnp.concatenate([high, low], axis=1)


def fold(wide):
    width = wide.shape[1] // 2
    return wide[:, :width] + wide[:, width:]


def twice(pair):
    return jnp.concatenate([pair, pair], axis=0)


def kernel(
    chain,
    gain_ref, ridge_ref, query_hbm, key_hbm, value_hbm, out_ref,
    query_ref, key_ref, value_ref,
    keys, turned_keys, gram_head, gram_all, cross_head, cross_all,
    gram_in, gram_out, gram_side, cross_in, cross_out, cross_mix, cross_half, cross_side,
    weights, start, solved, final,
    query_sem, key_sem, value_sem,
    gram_send, gram_recv, side_send, side_recv,
    cross_send, cross_recv, half_send, half_recv, cside_send, cside_recv,
):
    heads = keys.shape[0]
    tokens, dim = keys.shape[1:]
    sub = tokens // 2
    pairs = heads // 2
    place = lax.axis_index("seq")
    row, lane = place // LANES, place % LANES
    partner = place + 1 - 2 * lane
    has_prev, has_next = row > 0, row < chain - 1
    gets_side = jnp.logical_or(lane == 1, has_prev)

    barrier = pltpu.get_barrier_semaphore()

    def greet(device):
        pl.semaphore_signal(barrier, inc=1, device_id={"seq": device}, device_id_type=MESH)

    greet(partner)

    @pl.when(has_prev)
    def _():
        greet(place - LANES)

    @pl.when(has_next)
    def _():
        greet(place + LANES)

    def pair_cols(p):
        return slice(2 * p * dim, 2 * (p + 1) * dim)

    def fetch(p, src, dst, sem):
        return pltpu.make_async_copy(src.at[:, pair_cols(p)], dst.at[:, pair_cols(p)], sem.at[p])

    for p in range(pairs):
        fetch(p, key_hbm, key_ref, key_sem).start()
    for p in range(pairs):
        fetch(p, value_hbm, value_ref, value_sem).start()
    for p in range(pairs):
        fetch(p, query_hbm, query_ref, query_sem).start()

    i = lax.broadcasted_iota(jnp.int32, (dim, dim), 0)
    j = lax.broadcasted_iota(jnp.int32, (dim, dim), 1)
    eye = jnp.where(i == j, 1.0, 0.0).astype(F32)

    def copy(src, dst, send, recv, device):
        return pltpu.make_async_remote_copy(
            src_ref=src, dst_ref=dst, send_sem=send, recv_sem=recv,
            device_id={"seq": device}, device_id_type=MESH,
        )

    pieces = [(p, q) for p in range(pairs) for q in range(2)]
    spans = (slice(0, dim // 2), slice(dim // 2, dim + 8))

    def gram_next(p, q):
        n = 2 * p + q
        return copy(
            gram_out.at[p, spans[q]], gram_in.at[p, spans[q]],
            gram_send.at[n], gram_recv.at[n], place + LANES,
        )

    def gram_across(p, q, src):
        n = 2 * p + q
        return copy(
            src.at[p, spans[q]], gram_side.at[p, spans[q]],
            side_send.at[n], side_recv.at[n], partner,
        )

    def cross_next(p):
        return copy(cross_out.at[p], cross_in.at[p], cross_send.at[p], cross_recv.at[p], place + LANES)

    def cross_across(p, src):
        return copy(src.at[p], cross_side.at[p], cside_send.at[p], cside_recv.at[p], partner)

    def send_gram(p, q):
        @pl.when(has_next)
        def _():
            gram_next(p, q).start()

        @pl.when(lane == 0)
        def _():
            gram_across(p, q, gram_out).start()

    def cross_swap(p):
        return copy(
            cross_all.at[2 * p + 1 - lane], cross_half.at[p],
            half_send.at[p], half_recv.at[p], partner,
        )

    def relay_cross(p):
        cross_swap(p).wait_recv()

        @pl.when(has_prev)
        def _():
            cross_next(p).wait_recv()

            @pl.when(lane == 1)
            def _():
                cross_across(p, cross_in).start()

        mixed = cross_in[p] + cross_all[2 * p + lane]

        @pl.when(lane == 0)
        def _():
            cross_mix[p] = mixed
            cross_across(p, cross_mix).start()

        @pl.when(has_next)
        def _():
            cross_out[p] = mixed + cross_half[p]
            cross_next(p).start()

    for p in range(pairs):
        fetch(p, key_hbm, key_ref, key_sem).wait()
        for h in (2 * p, 2 * p + 1):
            raw = key_ref[:, h * dim : (h + 1) * dim].astype(F32)
            scaled = (raw * gain_ref[h]).astype(BF16)
            turned = scaled.T
            keys[h] = scaled
            turned_keys[h] = turned
            first = mm(turned[:, :sub], scaled[:sub])
            gram_head[h] = first
            gram_all[h] = first + mm(turned[:, sub:], scaled[sub:])
        upper, lower = gram_all[2 * p], gram_all[2 * p + 1]
        gram_out[p, :dim] = jnp.where(i <= j, upper, lower)
        diagonal = jnp.sum(jnp.where(i == j, lower, 0.0), axis=0, keepdims=True)
        gram_out[p, dim:] = jnp.broadcast_to(diagonal, (8, dim))
        if p == 0:
            pl.semaphore_wait(barrier, 1 + has_prev.astype(jnp.int32) + has_next.astype(jnp.int32))

        @pl.when(jnp.logical_not(has_prev))
        def _():
            for q in range(2):
                send_gram(p, q)

    for p in range(pairs):
        fetch(p, value_hbm, value_ref, value_sem).wait()
        for h in (2 * p, 2 * p + 1):
            values = value_ref[:, h * dim : (h + 1) * dim]
            first = mm(turned_keys[h, :, :sub], values[:sub])
            total = first + mm(turned_keys[h, :, sub:], values[sub:])
            cross_head[h] = first
            cross_all[h] = total
        cross_swap(p).start()

    @pl.when(jnp.logical_not(has_prev))
    def _():
        gram_in[...] = jnp.zeros_like(gram_in)
        cross_in[...] = jnp.zeros_like(cross_in)
        for p in range(pairs):
            relay_cross(p)

    @pl.when(jnp.logical_not(gets_side))
    def _():
        gram_side[...] = jnp.zeros_like(gram_side)
        cross_side[...] = jnp.zeros_like(cross_side)

    for p in range(pairs):
        fetch(p, query_hbm, query_ref, query_sem).wait()

    @pl.when(has_prev)
    def _():
        for p, q in pieces:
            gram_next(p, q).wait_recv()

            @pl.when(lane == 1)
            def _():
                gram_across(p, q, gram_in).start()

            gram_out[p, spans[q]] += gram_in[p, spans[q]]
            send_gram(p, q)

    def arrive(p):
        @pl.when(gets_side)
        def _():
            for q in range(2):
                gram_across(p, q, gram_in).wait_recv()

    def precondition(p, result):
        packed = gram_in[p] + gram_side[p]
        square = packed[:dim]
        turned = square.T
        upper = jnp.where(i <= j, square, turned)
        lower = jnp.where(i > j, square, jnp.where(i < j, turned, packed[dim : dim + 1]))
        state = []
        for h, prior in ((2 * p, upper), (2 * p + 1, lower)):
            plain = ridge_ref[h] * eye + prior
            gram_head[h] = plain + gram_head[h]
            end = plain + gram_all[h]
            gram_all[h] = plain
            total = jnp.sum(jnp.sum(end * end, axis=1, keepdims=True), axis=0, keepdims=True)
            inverse = 1.0 / jnp.sqrt(total)
            rest = eye - end * inverse
            split = halves(rest)
            both = jnp.concatenate([eye + rest, fold(mm(split, twice(split)))], axis=0)
            state.append((both, inverse))
        yield
        for step in range(NS_STEPS - 2):
            for k in range(2):
                both, inverse = state[k]
                split = halves(both)
                product = fold(mm(split, twice(split[dim:])))
                both = jnp.concatenate([both[:dim] + product[:dim], product[dim:]], axis=0)
                state[k] = (both, inverse)
            yield
        for both, inverse in state:
            split = halves(both)
            approx = both[:dim] + fold(mm(split[:dim], twice(split[dim:])))
            result.append(halves(approx * inverse))
        yield

    t = lax.broadcasted_iota(jnp.int32, (sub, sub), 0)
    u = lax.broadcasted_iota(jnp.int32, (sub, sub), 1)
    causal = t >= u

    def solve(p, preconds):
        slot = p % 2
        for k in range(2):
            h = 2 * p + k
            precond = preconds[k]
            start[slot, k] = fold(mm(query_ref[:, h * dim : (h + 1) * dim], precond))
            shifted = halves(-fold(mm(keys[h], precond)))
            for s, matrix in ((0, gram_all), (1, gram_head)):
                rest = halves(eye - fold(mm(halves(matrix[h]), twice(precond))))
                weights[slot, k, s, :sub] = shifted[s * sub : (s + 1) * sub]
                weights[slot, k, s, sub:] = twice(rest)
            yield
        chains = [(k, s) for k in range(2) for s in range(2)]
        current = {(k, s): start[slot, k, s * sub : (s + 1) * sub] for k, s in chains}
        for repeat in range(REFINE):
            for k, s in chains:
                rows = slice(s * sub, (s + 1) * sub)
                split = halves(current[k, s])
                scores = mm(split[:, :dim], turned_keys[2 * p + k, :, rows])
                scores = jnp.where(causal, scores, 0.0).astype(BF16)
                update = mm(jnp.concatenate([scores, split], axis=1), weights[slot, k, s])
                current[k, s] = start[slot, k, rows] + fold(update)
                if s == 1:
                    yield
        for k, s in chains:
            solved[2 * p + k, s * sub : (s + 1) * sub] = halves(current[k, s])

    def weave(*streams):
        streams = list(streams)
        while streams:
            streams = [stream for stream in streams if next(stream, 0) is None]

    def relay_at(stage):
        early = {0: (0, 1), 1: (2,), 2: range(3, pairs)}
        late = {1: (0,), 2: (1,), 3: range(2, pairs)}
        mine, spare = early.get(stage, ()), late.get(stage, ())

        @pl.when(jnp.logical_and(has_prev, has_next))
        def _():
            for p in mine:
                if p < pairs:
                    relay_cross(p)

        @pl.when(jnp.logical_and(has_prev, jnp.logical_not(has_next)))
        def _():
            for p in spare:
                if p < pairs:
                    relay_cross(p)

    arrive(0)
    preconds = []
    weave(precondition(0, preconds))
    for p in range(max(pairs, 4)):
        relay_at(p)
        if p >= pairs:
            continue
        later = []
        streams = [solve(p, preconds)]
        if p + 1 < pairs:
            arrive(p + 1)
            streams.append(precondition(p + 1, later))
        weave(*streams)
        preconds = later

    def read_pair(p, carry):
        @pl.when(gets_side)
        def _():
            cross_across(p, cross_in).wait_recv()

        for k in range(2):
            h = 2 * p + k
            cols = pl.ds(pl.multiple_of(h * dim, dim), dim)
            own = cross_in[p] + jnp.where(lane == 1, cross_half[p], 0.0)
            prior = jnp.where(lane == k, own, cross_side[p])
            for s in range(2):
                rows = slice(s * sub, (s + 1) * sub)
                values = value_ref[rows, cols]
                final[k, s, :sub] = jnp.concatenate([values, jnp.zeros_like(values)], axis=1)
                matrix = prior if s == 0 else prior + cross_head[h]
                final[k, s, sub:] = twice(halves(matrix))
                split = solved[h, rows]
                scores = mm(split[:, :dim], turned_keys[h, :, rows])
                scores = jnp.where(causal, scores, 0.0).astype(BF16)
                total = mm(jnp.concatenate([scores, split], axis=1), final[k, s])
                out_ref[rows, cols] = fold(total).astype(BF16)
        return carry

    lax.fori_loop(0, pairs, read_pair, 0)

    for p in range(pairs):
        cross_swap(p).wait_send()

        @pl.when(has_next)
        def _():
            for q in range(2):
                gram_next(p, q).wait_send()
            cross_next(p).wait_send()

        @pl.when(jnp.logical_or(lane == 0, has_prev))
        def _():
            for q in range(2):
                gram_across(p, q, gram_out).wait_send()
            cross_across(p, cross_out).wait_send()


def solution(mesh):
    chain = mesh.shape["seq"] // LANES

    def body(query_rows, key_rows, value_rows, key_gain, regularizer):
        heads = key_gain.shape[0]
        tokens, width = query_rows.shape
        dim = width // heads
        sub, pairs = tokens // 2, heads // 2
        vmem = pl.BlockSpec(memory_space=pltpu.VMEM)
        hbm = pl.BlockSpec(memory_space=pl.ANY)
        smem = pl.BlockSpec(memory_space=pltpu.SMEM)
        rows = pltpu.VMEM((tokens, width), BF16)
        square = pltpu.VMEM((heads, dim, dim), F32)
        packed = pltpu.VMEM((pairs, dim + 8, dim), F32)
        crosses = pltpu.VMEM((pairs, dim, dim), F32)
        return pl.pallas_call(
            functools.partial(kernel, chain),
            out_shape=pltpu.VMEM((tokens, width), BF16),
            in_specs=[smem, smem, hbm, hbm, hbm],
            out_specs=vmem,
            scratch_shapes=[
                rows, rows, rows,
                pltpu.VMEM((heads, tokens, dim), BF16),
                pltpu.VMEM((heads, dim, tokens), BF16),
                square, square, square, square,
                packed, packed, packed,
                crosses, crosses, crosses, crosses, crosses,
                pltpu.VMEM((2, 2, 2, sub + 2 * dim, 2 * dim), BF16),
                pltpu.VMEM((2, 2, tokens, dim), F32),
                pltpu.VMEM((heads, tokens, 2 * dim), BF16),
                pltpu.VMEM((2, 2, sub + 2 * dim, 2 * dim), BF16),
            ]
            + [pltpu.SemaphoreType.DMA((pairs,)) for _ in range(3)]
            + [pltpu.SemaphoreType.DMA((2 * pairs,)) for _ in range(4)]
            + [pltpu.SemaphoreType.DMA((pairs,)) for _ in range(6)],
            compiler_params=pltpu.CompilerParams(collective_id=0, has_side_effects=True),
            name="mesa_prefill",
        )(key_gain, regularizer, query_rows, key_rows, value_rows)

    placed = (P("seq", "head"), P("seq", "head"), P("seq", "head"), P("head"), P("head"))
    return jax.shard_map(
        body, mesh=mesh, in_specs=placed, out_specs=P("seq", "head"), check_vma=False
    )
```

```python
import functools

import jax
import jax.numpy as jnp
from jax import lax
from jax.experimental import pallas as pl
from jax.experimental.pallas import tpu as pltpu
from jax.sharding import PartitionSpec as P

NS_STEPS = 8
REFINE = 2
LANES = 2
F32 = jnp.float32
BF16 = jnp.bfloat16
MESH = pl.DeviceIdType.MESH


def mm(left, right):
    return lax.dot_general(left, right, (((1,), (0,)), ((), ())), preferred_element_type=F32)


def mm_nt(left, right):
    return lax.dot_general(left, right, (((1,), (1,)), ((), ())), preferred_element_type=F32)


def mm_tn(left, right):
    return lax.dot_general(left, right, (((0,), (0,)), ((), ())), preferred_element_type=F32)


def halves(value):
    high = value.astype(BF16)
    low = (value - high.astype(F32)).astype(BF16)
    return jnp.concatenate([high, low], axis=1)


def fold(wide):
    width = wide.shape[1] // 2
    return wide[:, :width] + wide[:, width:]


def twice(pair):
    return jnp.concatenate([pair, pair], axis=0)


def kernel(
    chain,
    gain_ref, ridge_ref, query_hbm, key_hbm, value_hbm, out_ref,
    query_ref, key_ref, value_ref,
    keys, turned_keys, gram_head, gram_all, cross_head, cross_all,
    gram_in, gram_out, gram_side, cross_in, cross_out, cross_mix, cross_half, cross_side,
    weights, start, solved, final,
    query_sem, key_sem, value_sem,
    gram_send, gram_recv, side_send, side_recv,
    cross_send, cross_recv, half_send, half_recv, cside_send, cside_recv,
):
    heads = keys.shape[0]
    tokens, dim = keys.shape[1:]
    sub = tokens // 2
    pairs = heads // 2
    place = lax.axis_index("seq")
    row, lane = place // LANES, place % LANES
    partner = place + 1 - 2 * lane
    has_prev, has_next = row > 0, row < chain - 1
    gets_side = jnp.logical_or(lane == 1, has_prev)

    barrier = pltpu.get_barrier_semaphore()

    def greet(device):
        pl.semaphore_signal(barrier, inc=1, device_id={"seq": device}, device_id_type=MESH)

    greet(partner)

    @pl.when(has_prev)
    def _():
        greet(place - LANES)

    @pl.when(has_next)
    def _():
        greet(place + LANES)

    def pair_cols(p):
        return slice(2 * p * dim, 2 * (p + 1) * dim)

    def fetch(p, src, dst, sem):
        return pltpu.make_async_copy(src.at[:, pair_cols(p)], dst.at[:, pair_cols(p)], sem.at[p])

    for p in range(pairs):
        fetch(p, key_hbm, key_ref, key_sem).start()
    for p in range(pairs):
        fetch(p, value_hbm, value_ref, value_sem).start()
    for p in range(pairs):
        fetch(p, query_hbm, query_ref, query_sem).start()

    i = lax.broadcasted_iota(jnp.int32, (dim, dim), 0)
    j = lax.broadcasted_iota(jnp.int32, (dim, dim), 1)
    eye = jnp.where(i == j, 1.0, 0.0).astype(F32)

    def copy(src, dst, send, recv, device):
        return pltpu.make_async_remote_copy(
            src_ref=src, dst_ref=dst, send_sem=send, recv_sem=recv,
            device_id={"seq": device}, device_id_type=MESH,
        )

    first_row = jnp.logical_not(has_prev)
    last_row = jnp.logical_and(has_prev, jnp.logical_not(has_next))
    middle = jnp.logical_and(has_prev, has_next)
    cuts = [dim // 4, dim // 2, 3 * dim // 4, dim + 8]
    quarters = [slice(a, b) for a, b in zip([0] + cuts[:-1], cuts)]
    halved = [slice(0, cuts[1]), slice(cuts[1], cuts[3])]
    spans = {(p, q): span for p in range(pairs) for q, span in enumerate(halved if p else quarters)}
    number = {piece: n for n, piece in enumerate(spans)}

    def pieces(p):
        return [q for k, q in spans if k == p]

    def gram_next(p, q):
        n = number[p, q]
        return copy(
            gram_out.at[p, spans[p, q]], gram_in.at[p, spans[p, q]],
            gram_send.at[n], gram_recv.at[n], place + LANES,
        )

    def gram_across(p, q, src):
        n = number[p, q]
        return copy(
            src.at[p, spans[p, q]], gram_side.at[p, spans[p, q]],
            side_send.at[n], side_recv.at[n], partner,
        )

    def cross_next(p):
        return copy(cross_out.at[p], cross_in.at[p], cross_send.at[p], cross_recv.at[p], place + LANES)

    def cross_across(p, src):
        return copy(src.at[p], cross_side.at[p], cside_send.at[p], cside_recv.at[p], partner)

    def send_side(p):
        @pl.when(jnp.logical_and(first_row, lane == 0))
        def _():
            for q in pieces(p):
                gram_across(p, q, gram_out).start()

    def relay_gram(p):
        for q in pieces(p):
            gram_next(p, q).wait_recv()

            @pl.when(lane == 1)
            def _():
                gram_across(p, q, gram_in).start()

            gram_out[p, spans[p, q]] += gram_in[p, spans[p, q]]

            @pl.when(has_next)
            def _():
                gram_next(p, q).start()

            @pl.when(lane == 0)
            def _():
                gram_across(p, q, gram_out).start()

    def cross_swap(p):
        return copy(
            cross_all.at[2 * p + 1 - lane], cross_half.at[p],
            half_send.at[p], half_recv.at[p], partner,
        )

    def relay_cross(p):
        cross_swap(p).wait_recv()

        @pl.when(has_prev)
        def _():
            cross_next(p).wait_recv()

            @pl.when(lane == 1)
            def _():
                cross_across(p, cross_in).start()

        mixed = cross_in[p] + cross_all[2 * p + lane]

        @pl.when(lane == 0)
        def _():
            cross_mix[p] = mixed
            cross_across(p, cross_mix).start()

        @pl.when(has_next)
        def _():
            cross_out[p] = mixed + cross_half[p]
            cross_next(p).start()

    for p in range(pairs):
        fetch(p, key_hbm, key_ref, key_sem).wait()
        for h in (2 * p, 2 * p + 1):
            raw = key_ref[:, h * dim : (h + 1) * dim].astype(F32)
            scaled = (raw * gain_ref[h]).astype(BF16)
            turned = scaled.T
            keys[h] = scaled
            turned_keys[h] = turned
            first = mm(turned[:, :sub], scaled[:sub])
            gram_head[h] = first
            gram_all[h] = first + mm(turned[:, sub:], scaled[sub:])
        upper, lower = gram_all[2 * p], gram_all[2 * p + 1]
        gram_out[p, :dim] = jnp.where(i <= j, upper, lower)
        diagonal = jnp.sum(jnp.where(i == j, lower, 0.0), axis=0, keepdims=True)
        gram_out[p, dim:] = jnp.broadcast_to(diagonal, (8, dim))
        if p == 0:
            pl.semaphore_wait(barrier, 1 + has_prev.astype(jnp.int32) + has_next.astype(jnp.int32))

        @pl.when(jnp.logical_and(first_row, has_next))
        def _():
            for q in pieces(p):
                gram_next(p, q).start()

        if p == 0:
            send_side(p)

    for p in range(pairs):
        fetch(p, value_hbm, value_ref, value_sem).wait()
        for h in (2 * p, 2 * p + 1):
            values = value_ref[:, h * dim : (h + 1) * dim]
            first = mm(turned_keys[h, :, :sub], values[:sub])
            total = first + mm(turned_keys[h, :, sub:], values[sub:])
            cross_head[h] = first
            cross_all[h] = total
        if p < 2:
            cross_swap(p).start()
        else:
            @pl.when(jnp.logical_not(middle))
            def _():
                cross_swap(p).start()
        if p == 1:
            send_side(1)
    for p in range(2, pairs):
        send_side(p)

    @pl.when(first_row)
    def _():
        gram_in[...] = jnp.zeros_like(gram_in)
        cross_in[...] = jnp.zeros_like(cross_in)

    @pl.when(jnp.logical_not(gets_side))
    def _():
        gram_side[...] = jnp.zeros_like(gram_side)
        cross_side[...] = jnp.zeros_like(cross_side)

    for p in range(pairs):
        fetch(p, query_hbm, query_ref, query_sem).wait()

    @pl.when(middle)
    def _():
        for p in range(pairs):
            relay_gram(p)
            if 1 <= p < pairs - 1:
                cross_swap(p + 1).start()

    @pl.when(last_row)
    def _():
        for p in range(min(2, pairs)):
            relay_gram(p)

    def arrive(p):
        @pl.when(gets_side)
        def _():
            for q in pieces(p):
                gram_across(p, q, gram_in).wait_recv()

    def precondition(p, result):
        packed = gram_in[p] + gram_side[p]
        square = packed[:dim]
        turned = square.T
        upper = jnp.where(i <= j, square, turned)
        lower = jnp.where(i > j, square, jnp.where(i < j, turned, packed[dim : dim + 1]))
        state = []
        for h, prior in ((2 * p, upper), (2 * p + 1, lower)):
            plain = ridge_ref[h] * eye + prior
            gram_head[h] = plain + gram_head[h]
            end = plain + gram_all[h]
            gram_all[h] = plain
            total = jnp.sum(jnp.sum(end * end, axis=1, keepdims=True), axis=0, keepdims=True)
            inverse = 1.0 / jnp.sqrt(total)
            rest = eye - end * inverse
            split = halves(rest)
            both = jnp.concatenate([eye + rest, fold(mm(split, twice(split)))], axis=0)
            state.append((both, inverse))
        yield
        for step in range(NS_STEPS - 2):
            for k in range(2):
                both, inverse = state[k]
                split = halves(both)
                product = fold(mm(split, twice(split[dim:])))
                both = jnp.concatenate([both[:dim] + product[:dim], product[dim:]], axis=0)
                state[k] = (both, inverse)
            yield
        for both, inverse in state:
            split = halves(both)
            approx = both[:dim] + fold(mm(split[:dim], twice(split[dim:])))
            result.append(halves(approx * inverse))
        yield

    t = lax.broadcasted_iota(jnp.int32, (sub, sub), 0)
    u = lax.broadcasted_iota(jnp.int32, (sub, sub), 1)
    causal = t >= u

    def solve(p, preconds):
        slot = p % 2
        for k in range(2):
            h = 2 * p + k
            precond = preconds[k]
            start[slot, k] = fold(mm(query_ref[:, h * dim : (h + 1) * dim], precond))
            shifted = halves(-fold(mm(keys[h], precond)))
            for s, matrix in ((0, gram_all), (1, gram_head)):
                rest = halves(eye - fold(mm(halves(matrix[h]), twice(precond))))
                weights[slot, k, s, :sub] = shifted[s * sub : (s + 1) * sub]
                weights[slot, k, s, sub:] = twice(rest)
            yield
        chains = [(k, s) for k in range(2) for s in range(2)]
        current = {(k, s): start[slot, k, s * sub : (s + 1) * sub] for k, s in chains}
        for repeat in range(REFINE):
            for k, s in chains:
                rows = slice(s * sub, (s + 1) * sub)
                split = halves(current[k, s])
                scores = mm(split[:, :dim], turned_keys[2 * p + k, :, rows])
                scores = jnp.where(causal, scores, 0.0).astype(BF16)
                update = mm(jnp.concatenate([scores, split], axis=1), weights[slot, k, s])
                current[k, s] = start[slot, k, rows] + fold(update)
                if s == 1:
                    yield
        for k, s in chains:
            solved[2 * p + k, s * sub : (s + 1) * sub] = halves(current[k, s])

    def weave(*streams):
        streams = list(streams)
        while streams:
            streams = [stream for stream in streams if next(stream, 0) is None]

    rows = jnp.minimum(row, 2)
    roles = (
        (first_row, (0, 0, 0, 0)),
        (jnp.logical_and(middle, rows == 1), (0, 0, 0, 1)),
        (jnp.logical_and(middle, rows == 2), (0, 1, 1, 2)),
        (last_row, (1, 2, 2, 3)),
    )
    end = pairs

    def relay_at(slot):
        for role, slots in roles:
            units = [p for p in range(pairs) if min(slots[min(p, 3)], end) == slot]
            if units:
                @pl.when(role)
                def _():
                    for p in units:
                        relay_cross(p)

    arrive(0)
    preconds = []
    weave(precondition(0, preconds))

    @pl.when(last_row)
    def _():
        for p in range(2, pairs):
            relay_gram(p)

    relay_at(0)
    for p in range(pairs):
        later = []
        streams = [solve(p, preconds)]
        if p + 1 < pairs:
            arrive(p + 1)
            streams.append(precondition(p + 1, later))
        weave(*streams)
        relay_at(p + 1)
        preconds = later

    def read_pair(p, carry):
        @pl.when(gets_side)
        def _():
            cross_across(p, cross_in).wait_recv()

        for k in range(2):
            h = 2 * p + k
            cols = pl.ds(pl.multiple_of(h * dim, dim), dim)
            own = cross_in[p] + jnp.where(lane == 1, cross_half[p], 0.0)
            prior = jnp.where(lane == k, own, cross_side[p])
            for s in range(2):
                rows = slice(s * sub, (s + 1) * sub)
                values = value_ref[rows, cols]
                final[k, s, :sub] = jnp.concatenate([values, jnp.zeros_like(values)], axis=1)
                matrix = prior if s == 0 else prior + cross_head[h]
                final[k, s, sub:] = twice(halves(matrix))
                split = solved[h, rows]
                scores = mm(split[:, :dim], turned_keys[h, :, rows])
                scores = jnp.where(causal, scores, 0.0).astype(BF16)
                total = mm(jnp.concatenate([scores, split], axis=1), final[k, s])
                out_ref[rows, cols] = fold(total).astype(BF16)
        return carry

    lax.fori_loop(0, pairs, read_pair, 0)

    for p in range(pairs):
        cross_swap(p).wait_send()

        @pl.when(has_next)
        def _():
            for q in pieces(p):
                gram_next(p, q).wait_send()
            cross_next(p).wait_send()

        @pl.when(jnp.logical_or(lane == 0, has_prev))
        def _():
            for q in pieces(p):
                gram_across(p, q, gram_out).wait_send()
            cross_across(p, cross_out).wait_send()


def solution(mesh):
    chain = mesh.shape["seq"] // LANES

    def body(query_rows, key_rows, value_rows, key_gain, regularizer):
        heads = key_gain.shape[0]
        tokens, width = query_rows.shape
        dim = width // heads
        sub, pairs = tokens // 2, heads // 2
        vmem = pl.BlockSpec(memory_space=pltpu.VMEM)
        hbm = pl.BlockSpec(memory_space=pl.ANY)
        smem = pl.BlockSpec(memory_space=pltpu.SMEM)
        rows = pltpu.VMEM((tokens, width), BF16)
        square = pltpu.VMEM((heads, dim, dim), F32)
        packed = pltpu.VMEM((pairs, dim + 8, dim), F32)
        crosses = pltpu.VMEM((pairs, dim, dim), F32)
        return pl.pallas_call(
            functools.partial(kernel, chain),
            out_shape=pltpu.VMEM((tokens, width), BF16),
            in_specs=[smem, smem, hbm, hbm, hbm],
            out_specs=vmem,
            scratch_shapes=[
                rows, rows, rows,
                pltpu.VMEM((heads, tokens, dim), BF16),
                pltpu.VMEM((heads, dim, tokens), BF16),
                square, square, square, square,
                packed, packed, packed,
                crosses, crosses, crosses, crosses, crosses,
                pltpu.VMEM((2, 2, 2, sub + 2 * dim, 2 * dim), BF16),
                pltpu.VMEM((2, 2, tokens, dim), F32),
                pltpu.VMEM((heads, tokens, 2 * dim), BF16),
                pltpu.VMEM((2, 2, sub + 2 * dim, 2 * dim), BF16),
            ]
            + [pltpu.SemaphoreType.DMA((pairs,)) for _ in range(3)]
            + [pltpu.SemaphoreType.DMA((2 * pairs + 2,)) for _ in range(4)]
            + [pltpu.SemaphoreType.DMA((pairs,)) for _ in range(6)],
            compiler_params=pltpu.CompilerParams(collective_id=0, has_side_effects=True),
            name="mesa_prefill",
        )(key_gain, regularizer, query_rows, key_rows, value_rows)

    placed = (P("seq", "head"), P("seq", "head"), P("seq", "head"), P("head"), P("head"))
    return jax.shard_map(
        body, mesh=mesh, in_specs=placed, out_specs=P("seq", "head"), check_vma=False
    )
```

```python
import functools

import jax
import jax.numpy as jnp
from jax import lax
from jax.experimental import pallas as pl
from jax.experimental.pallas import tpu as pltpu
from jax.sharding import PartitionSpec as P

NS_STEPS = 8
REFINE = 2
LANES = 2
PARTS = 4
GROUP = 1
F32 = jnp.float32
BF16 = jnp.bfloat16
MESH = pl.DeviceIdType.MESH


def mm(left, right):
    return lax.dot_general(left, right, (((1,), (0,)), ((), ())), preferred_element_type=F32)


def mm_nt(left, right):
    return lax.dot_general(left, right, (((1,), (1,)), ((), ())), preferred_element_type=F32)


def mm_tn(left, right):
    return lax.dot_general(left, right, (((0,), (0,)), ((), ())), preferred_element_type=F32)


def halves(value):
    high = value.astype(BF16)
    low = (value - high.astype(F32)).astype(BF16)
    return jnp.concatenate([high, low], axis=1)


def fold(wide):
    width = wide.shape[1] // 2
    return wide[:, :width] + wide[:, width:]


def twice(pair):
    return jnp.concatenate([pair, pair], axis=0)


def kernel(
    chain,
    gain_hbm, ridge_hbm, query_hbm, key_hbm, value_hbm, out_ref,
    gain_ref, ridge_ref,
    query_ref, key_ref, value_ref,
    keys, turned_keys, gram_parts, gram_all, cross_head, cross_all,
    gram_in, gram_out, gram_side, cross_in, cross_out, cross_mix, cross_half, cross_side,
    weights, start, solved, final,
    query_sem, key_sem, value_sem, gain_sem, ridge_sem,
    gram_send, gram_recv, side_send, side_recv,
    cross_send, cross_recv, half_send, half_recv, cside_send, cside_recv,
):
    heads, dim, tokens = turned_keys.shape
    sub, part = tokens // 2, tokens // PARTS
    pairs = heads // 2
    place = lax.axis_index("seq")
    row, lane = place // LANES, place % LANES
    partner = place + 1 - 2 * lane
    has_prev, has_next = row > 0, row < chain - 1
    gets_side = jnp.logical_or(lane == 1, has_prev)

    barrier = pltpu.get_barrier_semaphore()

    def greet(device):
        pl.semaphore_signal(barrier, inc=1, device_id={"seq": device}, device_id_type=MESH)

    greet(partner)

    @pl.when(has_prev)
    def _():
        greet(place - LANES)

    @pl.when(has_next)
    def _():
        greet(place + LANES)

    def pair_cols(p):
        return slice(2 * p * dim, 2 * (p + 1) * dim)

    def fetch(p, src, dst, sem):
        return pltpu.make_async_copy(src.at[:, pair_cols(p)], dst.at[:, pair_cols(p)], sem.at[p])

    gains = pltpu.make_async_copy(gain_hbm, gain_ref, gain_sem)
    ridges = pltpu.make_async_copy(ridge_hbm, ridge_ref, ridge_sem)
    fetch(0, key_hbm, key_ref, key_sem).start()
    gains.start()
    for p in range(1, pairs):
        fetch(p, key_hbm, key_ref, key_sem).start()
    ridges.start()
    for p in range(pairs):
        fetch(p, value_hbm, value_ref, value_sem).start()
    for p in range(pairs):
        fetch(p, query_hbm, query_ref, query_sem).start()

    i = lax.broadcasted_iota(jnp.int32, (dim, dim), 0)
    j = lax.broadcasted_iota(jnp.int32, (dim, dim), 1)
    eye = jnp.where(i == j, 1.0, 0.0).astype(F32)

    def copy(src, dst, send, recv, device):
        return pltpu.make_async_remote_copy(
            src_ref=src, dst_ref=dst, send_sem=send, recv_sem=recv,
            device_id={"seq": device}, device_id_type=MESH,
        )

    first_row = jnp.logical_not(has_prev)
    last_row = jnp.logical_and(has_prev, jnp.logical_not(has_next))
    middle = jnp.logical_and(has_prev, has_next)
    cuts = [dim // 4, dim // 2, 3 * dim // 4, dim + 8]
    quarters = [slice(a, b) for a, b in zip([0] + cuts[:-1], cuts)]
    halved = [slice(0, cuts[1]), slice(cuts[1], cuts[3])]
    spans = {(p, q): span for p in range(pairs) for q, span in enumerate(halved if p else quarters)}
    number = {piece: n for n, piece in enumerate(spans)}

    def pieces(p):
        return [q for k, q in spans if k == p]

    def gram_next(p, q):
        n = number[p, q]
        return copy(
            gram_out.at[p, spans[p, q]], gram_in.at[p, spans[p, q]],
            gram_send.at[n], gram_recv.at[n], place + LANES,
        )

    def gram_across(p, q, src):
        n = number[p, q]
        return copy(
            src.at[p, spans[p, q]], gram_side.at[p, spans[p, q]],
            side_send.at[n], side_recv.at[n], partner,
        )

    def cross_next(p):
        return copy(cross_out.at[p], cross_in.at[p], cross_send.at[p], cross_recv.at[p], place + LANES)

    def cross_across(p, src):
        return copy(src.at[p], cross_side.at[p], cside_send.at[p], cside_recv.at[p], partner)

    def send_side(p):
        @pl.when(jnp.logical_and(first_row, lane == 0))
        def _():
            for q in pieces(p):
                gram_across(p, q, gram_out).start()

    def relay_gram(p):
        for q in pieces(p):
            gram_next(p, q).wait_recv()

            @pl.when(lane == 1)
            def _():
                gram_across(p, q, gram_in).start()

            gram_out[p, spans[p, q]] += gram_in[p, spans[p, q]]

            @pl.when(has_next)
            def _():
                gram_next(p, q).start()

            @pl.when(lane == 0)
            def _():
                gram_across(p, q, gram_out).start()

    def cross_swap(p):
        return copy(
            cross_all.at[2 * p + 1 - lane], cross_half.at[p],
            half_send.at[p], half_recv.at[p], partner,
        )

    def swap_cross(p):
        @pl.when(jnp.logical_not(jnp.logical_and(last_row, lane == 1)))
        def _():
            cross_swap(p).start()

    def relay_cross(p):
        @pl.when(jnp.logical_not(jnp.logical_and(last_row, lane == 0)))
        def _():
            cross_swap(p).wait_recv()

        @pl.when(has_prev)
        def _():
            cross_next(p).wait_recv()

            @pl.when(lane == 1)
            def _():
                cross_across(p, cross_in).start()

        mixed = cross_in[p] + cross_all[2 * p + lane]

        @pl.when(lane == 0)
        def _():
            cross_mix[p] = mixed
            cross_across(p, cross_mix).start()

        @pl.when(has_next)
        def _():
            cross_out[p] = mixed + cross_half[p]
            cross_next(p).start()

    gains.wait()
    for p in range(pairs):
        fetch(p, key_hbm, key_ref, key_sem).wait()
        for h in (2 * p, 2 * p + 1):
            raw = key_ref[:, h * dim : (h + 1) * dim].astype(F32)
            scaled = (raw * gain_ref[h]).astype(BF16)
            turned = scaled.T
            keys[p, :, (h - 2 * p) * dim : (h - 2 * p + 1) * dim] = scaled
            turned_keys[h] = turned
            gram_all[h] = mm(turned, scaled)
        upper, lower = gram_all[2 * p], gram_all[2 * p + 1]
        gram_out[p, :dim] = jnp.where(i <= j, upper, lower)
        diagonal = jnp.sum(jnp.where(i == j, lower, 0.0), axis=0, keepdims=True)
        gram_out[p, dim:] = jnp.broadcast_to(diagonal, (8, dim))
        if p == 0:
            pl.semaphore_wait(barrier, 1 + has_prev.astype(jnp.int32) + has_next.astype(jnp.int32))

        @pl.when(jnp.logical_and(first_row, has_next))
        def _():
            for q in pieces(p):
                gram_next(p, q).start()

        if p == 0:
            send_side(p)

    for p in range(pairs):
        fetch(p, value_hbm, value_ref, value_sem).wait()
        for h in (2 * p, 2 * p + 1):
            values = value_ref[:, h * dim : (h + 1) * dim]
            first = mm(turned_keys[h, :, :sub], values[:sub])
            total = first + mm(turned_keys[h, :, sub:], values[sub:])
            cross_head[h] = first
            cross_all[h] = total
        if p < 2:
            swap_cross(p)
        else:
            @pl.when(jnp.logical_not(middle))
            def _():
                swap_cross(p)
        if p == 1:
            send_side(1)
    for p in range(2, pairs):
        send_side(p)

    @pl.when(first_row)
    def _():
        gram_in[...] = jnp.zeros_like(gram_in)
        cross_in[...] = jnp.zeros_like(cross_in)

    @pl.when(jnp.logical_and(last_row, lane == 0))
    def _():
        cross_half[...] = jnp.zeros_like(cross_half)

    @pl.when(jnp.logical_not(gets_side))
    def _():
        gram_side[...] = jnp.zeros_like(gram_side)
        cross_side[...] = jnp.zeros_like(cross_side)

    ridges.wait()
    for p in range(pairs):
        fetch(p, query_hbm, query_ref, query_sem).wait()

    second_row = jnp.logical_and(middle, row == 1)

    @pl.when(second_row)
    def _():
        relay_gram(0)

    weights[:, :, :, :part, dim:] = jnp.zeros((2, 2, PARTS, part, dim), BF16)
    for h in range(heads):
        total = None
        for s in range(PARTS - 1):
            rows = slice(s * part, (s + 1) * part)
            cols = slice(h % 2 * dim, (h % 2 + 1) * dim)
            gram = mm(turned_keys[h, :, rows], keys[h // 2, rows, cols])
            total = gram if total is None else total + gram
            gram_parts[h, s * dim : (s + 1) * dim] = halves(total)

    @pl.when(jnp.logical_and(middle, row > 1))
    def _():
        relay_gram(0)

    @pl.when(middle)
    def _():
        for p in range(1, pairs):
            relay_gram(p)
            if p < pairs - 1:
                cross_swap(p + 1).start()

    @pl.when(last_row)
    def _():
        for p in range(min(2, pairs)):
            relay_gram(p)

    def arrive(p):
        @pl.when(gets_side)
        def _():
            for q in pieces(p):
                gram_across(p, q, gram_in).wait_recv()

    def precondition(p, result):
        packed = gram_in[p] + gram_side[p]
        square = packed[:dim]
        turned = square.T
        upper = jnp.where(i <= j, square, turned)
        lower = jnp.where(i > j, square, jnp.where(i < j, turned, packed[dim : dim + 1]))
        state = []
        for h, prior in ((2 * p, upper), (2 * p + 1, lower)):
            plain = ridge_ref[h] * eye + prior
            end = plain + gram_all[h]
            gram_all[h] = plain
            total = jnp.sum(jnp.sum(end * end, axis=1, keepdims=True), axis=0, keepdims=True)
            inverse = 1.0 / jnp.sqrt(total)
            rest = eye - end * inverse
            split = halves(rest)
            both = jnp.concatenate([fold(mm(split, twice(split))), eye + rest], axis=0)
            state.append((both, inverse))
        yield
        for step in range(NS_STEPS - 2):
            for k in range(2):
                both, inverse = state[k]
                split = halves(both)
                product = fold(mm(split, twice(split[:dim])))
                both = jnp.concatenate([product[:dim], both[dim:] + product[dim:]], axis=0)
                state[k] = (both, inverse)
            yield
        for both, inverse in state:
            split = halves(both)
            approx = both[dim:] + fold(mm(split[dim:], twice(split[:dim])))
            result.append(halves(approx * inverse))
        yield

    def causal(size):
        t = lax.broadcasted_iota(jnp.int32, (size, size), 0)
        u = lax.broadcasted_iota(jnp.int32, (size, size), 1)
        return t >= u

    def solve(p, preconds):
        slot = p % 2
        blank = jnp.zeros((dim, dim), BF16)
        both = jnp.concatenate([
            jnp.concatenate([preconds[0][:, :dim], blank], axis=1),
            jnp.concatenate([blank, preconds[1][:, :dim]], axis=1),
        ], axis=0)
        shifted = (-mm(keys[p], both)).astype(BF16)
        scores, current = {}, {}

        def prepare(k):
            h = 2 * p + k
            precond = preconds[k]
            start[slot, k] = fold(mm(query_ref[:, h * dim : (h + 1) * dim], precond))
            stack = jnp.concatenate([halves(gram_all[h]), gram_parts[h]], axis=0)
            product = fold(mm(stack, twice(precond)))
            rest = eye - product[:dim]
            for s in range(PARTS):
                left = rest - product[s * dim : (s + 1) * dim] if s else rest
                weights[slot, k, s, :part, :dim] = shifted[s * part : (s + 1) * part, k * dim : (k + 1) * dim]
                weights[slot, k, s, part:] = halves(left)
                current[k, s] = start[slot, k, s * part : (s + 1) * part].astype(BF16)

        def score(k):
            for s in range(PARTS):
                product = mm(current[k, s], turned_keys[2 * p + k, :, s * part : (s + 1) * part])
                scores[k, s] = jnp.where(causal(part), product, 0.0).astype(BF16)

        def update(k, last):
            for s in range(PARTS):
                rows = slice(s * part, (s + 1) * part)
                both = jnp.concatenate([scores[k, s], current[k, s]], axis=1)
                value = start[slot, k, rows] + fold(mm(both, weights[slot, k, s]))
                if last:
                    solved[2 * p + k, rows] = halves(value)
                else:
                    current[k, s] = value.astype(BF16)

        prepare(0)
        yield
        prepare(1)
        score(0)
        yield
        for repeat in range(REFINE):
            last = repeat == REFINE - 1
            update(0, last)
            score(1)
            yield
            update(1, last)
            if not last:
                score(0)
            yield

    def weave(*streams):
        streams = list(streams)
        while streams:
            streams = [stream for stream in streams if next(stream, 0) is None]

    rows = jnp.minimum(row, 2)
    roles = (
        (first_row, (0, 0, 0, 0)),
        (jnp.logical_and(middle, rows == 1), (0, 0, 0, 1)),
        (jnp.logical_and(middle, rows == 2), (0, 1, 1, 2)),
        (last_row, (1, 2, 2, 3)),
    )
    end = pairs

    def relay_at(slot):
        for role, slots in roles:
            units = [p for p in range(pairs) if min(slots[min(p, 3)], end) == slot]
            if units:
                @pl.when(role)
                def _():
                    for p in units:
                        relay_cross(p)

    arrive(0)

    @pl.when(last_row)
    def _():
        for p in range(2, min(3, pairs)):
            relay_gram(p)

    preconds = []
    weave(precondition(0, preconds))

    @pl.when(last_row)
    def _():
        for p in range(3, pairs):
            relay_gram(p)

    relay_at(0)
    for p in range(pairs):
        later = []
        streams = [solve(p, preconds)]
        if p + 1 < pairs:
            arrive(p + 1)
            streams.append(precondition(p + 1, later))
        weave(*streams)
        relay_at(p + 1)
        preconds = later

    def read(turn, carry):
        for n in range(GROUP):
            @pl.when(gets_side)
            def _():
                cross_across(turn * GROUP + n, cross_in).wait_recv()

        for n, k in [(n, k) for n in range(GROUP) for k in range(2)]:
            p = turn * GROUP + n
            h = 2 * p + k
            cols = pl.ds(pl.multiple_of(h * dim, dim), dim)
            own = cross_in[p] + jnp.where(lane == 1, cross_half[p], 0.0)
            prior = jnp.where(lane == k, own, cross_side[p])
            for s in range(2):
                rows = slice(s * sub, (s + 1) * sub)
                values = value_ref[rows, cols]
                final[n, k, s, :sub] = jnp.concatenate([values, jnp.zeros_like(values)], axis=1)
                matrix = prior if s == 0 else prior + cross_head[h]
                final[n, k, s, sub:] = twice(halves(matrix))
                split = solved[h, rows]
                scores = mm(split[:, :dim], turned_keys[h, :, rows])
                scores = jnp.where(causal(sub), scores, 0.0).astype(BF16)
                total = mm(jnp.concatenate([scores, split], axis=1), final[n, k, s])
                out_ref[rows, cols] = fold(total).astype(BF16)
        return carry

    lax.fori_loop(0, pairs // GROUP, read, 0)

    for p in range(pairs):
        @pl.when(jnp.logical_not(jnp.logical_and(last_row, lane == 1)))
        def _():
            cross_swap(p).wait_send()

        @pl.when(has_next)
        def _():
            for q in pieces(p):
                gram_next(p, q).wait_send()
            cross_next(p).wait_send()

        @pl.when(jnp.logical_or(lane == 0, has_prev))
        def _():
            for q in pieces(p):
                gram_across(p, q, gram_out).wait_send()
            cross_across(p, cross_out).wait_send()


def solution(mesh):
    chain = mesh.shape["seq"] // LANES

    def body(query_rows, key_rows, value_rows, key_gain, regularizer):
        heads = key_gain.shape[0]
        tokens, width = query_rows.shape
        dim = width // heads
        sub, pairs = tokens // 2, heads // 2
        vmem = pl.BlockSpec(memory_space=pltpu.VMEM)
        hbm = pl.BlockSpec(memory_space=pl.ANY)
        rows = pltpu.VMEM((tokens, width), BF16)
        square = pltpu.VMEM((heads, dim, dim), F32)
        packed = pltpu.VMEM((pairs, dim + 8, dim), F32)
        crosses = pltpu.VMEM((pairs, dim, dim), F32)
        return pl.pallas_call(
            functools.partial(kernel, chain),
            out_shape=pltpu.VMEM((tokens, width), BF16),
            in_specs=[hbm] * 5,
            out_specs=vmem,
            scratch_shapes=[
                pltpu.SMEM((heads,), F32), pltpu.SMEM((heads,), F32),
                rows, rows, rows,
                pltpu.VMEM((pairs, tokens, 2 * dim), BF16),
                pltpu.VMEM((heads, dim, tokens), BF16),
                pltpu.VMEM((heads, (PARTS - 1) * dim, 2 * dim), BF16),
                square, square, square,
                packed, packed, packed,
                crosses, crosses, crosses, crosses, crosses,
                pltpu.VMEM((2, 2, PARTS, tokens // PARTS + dim, 2 * dim), BF16),
                pltpu.VMEM((2, 2, tokens, dim), F32),
                pltpu.VMEM((heads, tokens, 2 * dim), BF16),
                pltpu.VMEM((GROUP, 2, 2, sub + 2 * dim, 2 * dim), BF16),
            ]
            + [pltpu.SemaphoreType.DMA((pairs,)) for _ in range(3)]
            + [pltpu.SemaphoreType.DMA] * 2
            + [pltpu.SemaphoreType.DMA((2 * pairs + 2,)) for _ in range(4)]
            + [pltpu.SemaphoreType.DMA((pairs,)) for _ in range(6)],
            compiler_params=pltpu.CompilerParams(collective_id=0, has_side_effects=True),
            name="mesa_prefill",
        )(key_gain, regularizer, query_rows, key_rows, value_rows)

    placed = (P("seq", "head"), P("seq", "head"), P("seq", "head"), P("head"), P("head"))
    return jax.shard_map(
        body, mesh=mesh, in_specs=placed, out_specs=P("seq", "head"), check_vma=False
    )
```

```python
import functools

import jax
import jax.numpy as jnp
from jax import lax
from jax.experimental import pallas as pl
from jax.experimental.pallas import tpu as pltpu
from jax.sharding import PartitionSpec as P

NS_STEPS = 8
REFINE = 2
LANES = 2
PARTS = 4
GROUP = 1
F32 = jnp.float32
BF16 = jnp.bfloat16
MESH = pl.DeviceIdType.MESH


def mm(left, right):
    return lax.dot_general(left, right, (((1,), (0,)), ((), ())), preferred_element_type=F32)


def mm_nt(left, right):
    return lax.dot_general(left, right, (((1,), (1,)), ((), ())), preferred_element_type=F32)


def mm_tn(left, right):
    return lax.dot_general(left, right, (((0,), (0,)), ((), ())), preferred_element_type=F32)


def halves(value):
    high = value.astype(BF16)
    low = (value - high.astype(F32)).astype(BF16)
    return jnp.concatenate([high, low], axis=1)


def fold(wide):
    width = wide.shape[1] // 2
    return wide[:, :width] + wide[:, width:]


def twice(pair):
    return jnp.concatenate([pair, pair], axis=0)


def kernel(
    chain,
    gain_hbm, ridge_hbm, query_hbm, key_hbm, value_hbm, out_ref,
    gain_ref, ridge_ref,
    query_ref, key_ref, value_ref,
    keys, turned_keys, gram_parts, gram_all, cross_head, cross_all,
    gram_in, gram_out, gram_side, cross_in, cross_out, cross_mix, cross_half, cross_side,
    weights, start, solved, final,
    query_sem, key_sem, value_sem, gain_sem, ridge_sem,
    gram_send, gram_recv, side_send, side_recv,
    cross_send, cross_recv, half_send, half_recv, cside_send, cside_recv,
):
    heads, dim, tokens = turned_keys.shape
    sub, part = tokens // 2, tokens // PARTS
    pairs = heads // 2
    place = lax.axis_index("seq")
    row, lane = place // LANES, place % LANES
    partner = place + 1 - 2 * lane
    has_prev, has_next = row > 0, row < chain - 1
    gets_side = jnp.logical_or(lane == 1, has_prev)

    barrier = pltpu.get_barrier_semaphore()

    def greet(device):
        pl.semaphore_signal(barrier, inc=1, device_id={"seq": device}, device_id_type=MESH)

    greet(partner)

    @pl.when(has_prev)
    def _():
        greet(place - LANES)

    @pl.when(has_next)
    def _():
        greet(place + LANES)

    def pair_cols(p):
        return slice(2 * p * dim, 2 * (p + 1) * dim)

    def fetch(p, src, dst, sem):
        return pltpu.make_async_copy(src.at[:, pair_cols(p)], dst.at[:, pair_cols(p)], sem.at[p])

    gains = pltpu.make_async_copy(gain_hbm, gain_ref, gain_sem)
    ridges = pltpu.make_async_copy(ridge_hbm, ridge_ref, ridge_sem)
    fetch(0, key_hbm, key_ref, key_sem).start()
    gains.start()
    for p in range(1, pairs):
        fetch(p, key_hbm, key_ref, key_sem).start()
    ridges.start()
    values_in = pltpu.make_async_copy(value_hbm, value_ref, value_sem)
    queries_in = pltpu.make_async_copy(query_hbm, query_ref, query_sem)
    values_in.start()
    queries_in.start()

    i = lax.broadcasted_iota(jnp.int32, (dim, dim), 0)
    j = lax.broadcasted_iota(jnp.int32, (dim, dim), 1)
    eye = jnp.where(i == j, 1.0, 0.0).astype(F32)

    def copy(src, dst, send, recv, device):
        return pltpu.make_async_remote_copy(
            src_ref=src, dst_ref=dst, send_sem=send, recv_sem=recv,
            device_id={"seq": device}, device_id_type=MESH,
        )

    first_row = jnp.logical_not(has_prev)
    last_row = jnp.logical_and(has_prev, jnp.logical_not(has_next))
    middle = jnp.logical_and(has_prev, has_next)
    cuts = [dim // 4, dim // 2, 3 * dim // 4, dim + 8]
    quarters = [slice(a, b) for a, b in zip([0] + cuts[:-1], cuts)]
    halved = [slice(0, cuts[1]), slice(cuts[1], cuts[3])]
    spans = {(p, q): span for p in range(pairs) for q, span in enumerate(halved if p else quarters)}
    number = {piece: n for n, piece in enumerate(spans)}

    def pieces(p):
        return [q for k, q in spans if k == p]

    def gram_next(p, q):
        n = number[p, q]
        return copy(
            gram_out.at[p, spans[p, q]], gram_in.at[p, spans[p, q]],
            gram_send, gram_recv.at[n], place + LANES,
        )

    def gram_across(p, q, src):
        return copy(
            src.at[p, spans[p, q]], gram_side.at[p, spans[p, q]],
            side_send, side_recv.at[p], partner,
        )

    def side_of(p):
        return copy(gram_out.at[p], gram_side.at[p], side_send, side_recv.at[p], partner)

    def cross_next(p):
        return copy(cross_out.at[p], cross_in.at[p], cross_send, cross_recv.at[p], place + LANES)

    def cross_across(p, src):
        return copy(src.at[p], cross_side.at[p], cside_send, cside_recv.at[p], partner)

    def send_side(p):
        @pl.when(jnp.logical_and(first_row, lane == 0))
        def _():
            for q in pieces(p):
                gram_across(p, q, gram_out).start()

    def relay_gram(p):
        for q in pieces(p):
            gram_next(p, q).wait_recv()

            @pl.when(lane == 1)
            def _():
                gram_across(p, q, gram_in).start()

            gram_out[p, spans[p, q]] += gram_in[p, spans[p, q]]

            @pl.when(has_next)
            def _():
                gram_next(p, q).start()

            @pl.when(lane == 0)
            def _():
                gram_across(p, q, gram_out).start()

    def cross_swap(p):
        return copy(
            cross_all.at[2 * p + 1 - lane], cross_half.at[p],
            half_send, half_recv.at[p], partner,
        )

    def swap_cross(p):
        @pl.when(jnp.logical_not(jnp.logical_and(last_row, lane == 1)))
        def _():
            cross_swap(p).start()

    def relay_cross(p):
        @pl.when(jnp.logical_not(jnp.logical_and(last_row, lane == 0)))
        def _():
            cross_swap(p).wait_recv()

        @pl.when(has_prev)
        def _():
            cross_next(p).wait_recv()

            @pl.when(lane == 1)
            def _():
                cross_across(p, cross_in).start()

        mixed = cross_in[p] + cross_all[2 * p + lane]

        @pl.when(lane == 0)
        def _():
            cross_mix[p] = mixed
            cross_across(p, cross_mix).start()

        @pl.when(has_next)
        def _():
            cross_out[p] = mixed + cross_half[p]
            cross_next(p).start()

    gains.wait()
    for p in range(pairs):
        fetch(p, key_hbm, key_ref, key_sem).wait()
        for h in (2 * p, 2 * p + 1):
            raw = key_ref[:, h * dim : (h + 1) * dim].astype(F32)
            scaled = (raw * gain_ref[h]).astype(BF16)
            turned = scaled.T
            keys[p, :, (h - 2 * p) * dim : (h - 2 * p + 1) * dim] = scaled
            turned_keys[h] = turned
            gram_all[h] = mm(turned, scaled)
        upper, lower = gram_all[2 * p], gram_all[2 * p + 1]
        gram_out[p, :dim] = jnp.where(i <= j, upper, lower)
        diagonal = jnp.sum(jnp.where(i == j, lower, 0.0), axis=0, keepdims=True)
        gram_out[p, dim:] = jnp.broadcast_to(diagonal, (8, dim))
        if p == 0:
            pl.semaphore_wait(barrier, 1 + has_prev.astype(jnp.int32) + has_next.astype(jnp.int32))

        @pl.when(jnp.logical_and(first_row, has_next))
        def _():
            for q in pieces(p):
                gram_next(p, q).start()

        if p == 0:
            send_side(p)

    values_in.wait()
    for p in range(pairs):
        for h in (2 * p, 2 * p + 1):
            values = value_ref[:, h * dim : (h + 1) * dim]
            first = mm(turned_keys[h, :, :sub], values[:sub])
            total = first + mm(turned_keys[h, :, sub:], values[sub:])
            cross_head[h] = first
            cross_all[h] = total
        if p < 2:
            swap_cross(p)
        else:
            @pl.when(jnp.logical_not(middle))
            def _():
                swap_cross(p)
    for p in range(1, pairs):
        send_side(p)

    @pl.when(first_row)
    def _():
        gram_in[...] = jnp.zeros_like(gram_in)
        cross_in[...] = jnp.zeros_like(cross_in)

    @pl.when(jnp.logical_and(last_row, lane == 0))
    def _():
        cross_half[...] = jnp.zeros_like(cross_half)

    @pl.when(jnp.logical_not(gets_side))
    def _():
        gram_side[...] = jnp.zeros_like(gram_side)
        cross_side[...] = jnp.zeros_like(cross_side)

    ridges.wait()
    queries_in.wait()

    second_row = jnp.logical_and(middle, row == 1)

    @pl.when(second_row)
    def _():
        relay_gram(0)

    weights[:, :, :, :part, dim:] = jnp.zeros((2, 2, PARTS, part, dim), BF16)
    for h in range(heads):
        total = None
        for s in range(PARTS - 1):
            rows = slice(s * part, (s + 1) * part)
            cols = slice(h % 2 * dim, (h % 2 + 1) * dim)
            gram = mm(turned_keys[h, :, rows], keys[h // 2, rows, cols])
            total = gram if total is None else total + gram
            gram_parts[h, s * dim : (s + 1) * dim] = halves(total)

    @pl.when(jnp.logical_and(middle, row > 1))
    def _():
        relay_gram(0)

    @pl.when(middle)
    def _():
        for p in range(1, pairs):
            relay_gram(p)
            if p < pairs - 1:
                cross_swap(p + 1).start()

    @pl.when(last_row)
    def _():
        for p in range(min(2, pairs)):
            relay_gram(p)

    def arrive(p):
        @pl.when(gets_side)
        def _():
            side_of(p).wait_recv()

    def precondition(p, result):
        packed = gram_in[p] + gram_side[p]
        square = packed[:dim]
        turned = square.T
        upper = jnp.where(i <= j, square, turned)
        lower = jnp.where(i > j, square, jnp.where(i < j, turned, packed[dim : dim + 1]))
        state = []
        for h, prior in ((2 * p, upper), (2 * p + 1, lower)):
            plain = ridge_ref[h] * eye + prior
            end = plain + gram_all[h]
            gram_all[h] = plain
            total = jnp.sum(jnp.sum(end * end, axis=1, keepdims=True), axis=0, keepdims=True)
            inverse = 1.0 / jnp.sqrt(total)
            rest = eye - end * inverse
            split = halves(rest)
            both = jnp.concatenate([fold(mm(split, twice(split))), eye + rest], axis=0)
            state.append((both, inverse))
        yield
        for step in range(NS_STEPS - 2):
            for k in range(2):
                both, inverse = state[k]
                split = halves(both)
                product = fold(mm(split, twice(split[:dim])))
                both = jnp.concatenate([product[:dim], both[dim:] + product[dim:]], axis=0)
                state[k] = (both, inverse)
            yield
        for both, inverse in state:
            split = halves(both)
            approx = both[dim:] + fold(mm(split[dim:], twice(split[:dim])))
            result.append(halves(approx * inverse))
        yield

    def causal(size):
        t = lax.broadcasted_iota(jnp.int32, (size, size), 0)
        u = lax.broadcasted_iota(jnp.int32, (size, size), 1)
        return t >= u

    def solve(p, preconds):
        slot = p % 2
        blank = jnp.zeros((dim, dim), BF16)
        both = jnp.concatenate([
            jnp.concatenate([preconds[0][:, :dim], blank], axis=1),
            jnp.concatenate([blank, preconds[1][:, :dim]], axis=1),
        ], axis=0)
        shifted = (-mm(keys[p], both)).astype(BF16)
        scores, current = {}, {}

        def prepare(k):
            h = 2 * p + k
            precond = preconds[k]
            start[slot, k] = fold(mm(query_ref[:, h * dim : (h + 1) * dim], precond))
            stack = jnp.concatenate([halves(gram_all[h]), gram_parts[h]], axis=0)
            product = fold(mm(stack, twice(precond)))
            rest = eye - product[:dim]
            for s in range(PARTS):
                left = rest - product[s * dim : (s + 1) * dim] if s else rest
                weights[slot, k, s, :part, :dim] = shifted[s * part : (s + 1) * part, k * dim : (k + 1) * dim]
                weights[slot, k, s, part:] = halves(left)
                current[k, s] = start[slot, k, s * part : (s + 1) * part].astype(BF16)

        def score(k):
            for s in range(PARTS):
                product = mm(current[k, s], turned_keys[2 * p + k, :, s * part : (s + 1) * part])
                scores[k, s] = jnp.where(causal(part), product, 0.0).astype(BF16)

        def update(k, last):
            for s in range(PARTS):
                rows = slice(s * part, (s + 1) * part)
                both = jnp.concatenate([scores[k, s], current[k, s]], axis=1)
                value = start[slot, k, rows] + fold(mm(both, weights[slot, k, s]))
                if last:
                    solved[2 * p + k, rows] = halves(value)
                else:
                    current[k, s] = value.astype(BF16)

        prepare(0)
        yield
        prepare(1)
        score(0)
        yield
        for repeat in range(REFINE):
            last = repeat == REFINE - 1
            update(0, last)
            score(1)
            yield
            update(1, last)
            if not last:
                score(0)
            yield

    def weave(*streams):
        streams = list(streams)
        while streams:
            streams = [stream for stream in streams if next(stream, 0) is None]

    rows = jnp.minimum(row, 2)
    roles = (
        (first_row, (0, 0, 0, 0)),
        (jnp.logical_and(middle, rows == 1), (0, 0, 0, 1)),
        (jnp.logical_and(middle, rows == 2), (0, 1, 1, 2)),
        (last_row, (1, 2, 2, 3)),
    )
    end = pairs

    def relay_at(slot):
        for role, slots in roles:
            units = [p for p in range(pairs) if min(slots[min(p, 3)], end) == slot]
            if units:
                @pl.when(role)
                def _():
                    for p in units:
                        relay_cross(p)

    arrive(0)

    @pl.when(last_row)
    def _():
        for p in range(2, min(3, pairs)):
            relay_gram(p)

    preconds = []
    weave(precondition(0, preconds))

    @pl.when(last_row)
    def _():
        for p in range(3, pairs):
            relay_gram(p)

    relay_at(0)
    for p in range(pairs):
        later = []
        streams = [solve(p, preconds)]
        if p + 1 < pairs:
            arrive(p + 1)
            streams.append(precondition(p + 1, later))
        weave(*streams)
        relay_at(p + 1)
        preconds = later

    def read(turn, carry):
        for n in range(GROUP):
            @pl.when(gets_side)
            def _():
                cross_across(turn * GROUP + n, cross_in).wait_recv()

        for n, k in [(n, k) for n in range(GROUP) for k in range(2)]:
            p = turn * GROUP + n
            h = 2 * p + k
            cols = pl.ds(pl.multiple_of(h * dim, dim), dim)
            own = cross_in[p] + jnp.where(lane == 1, cross_half[p], 0.0)
            prior = jnp.where(lane == k, own, cross_side[p])
            for s in range(2):
                rows = slice(s * sub, (s + 1) * sub)
                values = value_ref[rows, cols]
                final[n, k, s, :sub] = jnp.concatenate([values, jnp.zeros_like(values)], axis=1)
                matrix = prior if s == 0 else prior + cross_head[h]
                final[n, k, s, sub:] = twice(halves(matrix))
                split = solved[h, rows]
                scores = mm(split[:, :dim], turned_keys[h, :, rows])
                scores = jnp.where(causal(sub), scores, 0.0).astype(BF16)
                total = mm(jnp.concatenate([scores, split], axis=1), final[n, k, s])
                out_ref[rows, cols] = fold(total).astype(BF16)
        return carry

    lax.fori_loop(0, pairs // GROUP, read, 0)

    @pl.when(jnp.logical_not(jnp.logical_and(last_row, lane == 1)))
    def _():
        copy(cross_out, cross_half, half_send, half_recv.at[0], partner).wait_send()

    @pl.when(has_next)
    def _():
        copy(gram_out, gram_in, gram_send, gram_recv.at[0], place + LANES).wait_send()
        copy(cross_out, cross_in, cross_send, cross_recv.at[0], place + LANES).wait_send()

    @pl.when(jnp.logical_or(lane == 0, has_prev))
    def _():
        copy(gram_out, gram_side, side_send, side_recv.at[0], partner).wait_send()
        copy(cross_out, cross_side, cside_send, cside_recv.at[0], partner).wait_send()


def solution(mesh):
    chain = mesh.shape["seq"] // LANES

    def body(query_rows, key_rows, value_rows, key_gain, regularizer):
        heads = key_gain.shape[0]
        tokens, width = query_rows.shape
        dim = width // heads
        sub, pairs = tokens // 2, heads // 2
        vmem = pl.BlockSpec(memory_space=pltpu.VMEM)
        hbm = pl.BlockSpec(memory_space=pl.ANY)
        rows = pltpu.VMEM((tokens, width), BF16)
        square = pltpu.VMEM((heads, dim, dim), F32)
        packed = pltpu.VMEM((pairs, dim + 8, dim), F32)
        crosses = pltpu.VMEM((pairs, dim, dim), F32)
        single = pltpu.SemaphoreType.DMA
        return pl.pallas_call(
            functools.partial(kernel, chain),
            out_shape=pltpu.VMEM((tokens, width), BF16),
            in_specs=[hbm] * 5,
            out_specs=vmem,
            scratch_shapes=[
                pltpu.SMEM((heads,), F32), pltpu.SMEM((heads,), F32),
                rows, rows, rows,
                pltpu.VMEM((pairs, tokens, 2 * dim), BF16),
                pltpu.VMEM((heads, dim, tokens), BF16),
                pltpu.VMEM((heads, (PARTS - 1) * dim, 2 * dim), BF16),
                square, square, square,
                packed, packed, packed,
                crosses, crosses, crosses, crosses, crosses,
                pltpu.VMEM((2, 2, PARTS, tokens // PARTS + dim, 2 * dim), BF16),
                pltpu.VMEM((2, 2, tokens, dim), F32),
                pltpu.VMEM((heads, tokens, 2 * dim), BF16),
                pltpu.VMEM((GROUP, 2, 2, sub + 2 * dim, 2 * dim), BF16),
            ]
            + [single, pltpu.SemaphoreType.DMA((pairs,))] + [single] * 3
            + [single, pltpu.SemaphoreType.DMA((2 * pairs + 2,))]
            + [single, pltpu.SemaphoreType.DMA((pairs,))] * 4,
            compiler_params=pltpu.CompilerParams(collective_id=0, has_side_effects=True),
            name="mesa_prefill",
        )(key_gain, regularizer, query_rows, key_rows, value_rows)

    placed = (P("seq", "head"), P("seq", "head"), P("seq", "head"), P("head"), P("head"))
    return jax.shard_map(
        body, mesh=mesh, in_specs=placed, out_specs=P("seq", "head"), check_vma=False
    )
```

```python
import functools

import jax
import jax.numpy as jnp
from jax import lax
from jax.experimental import pallas as pl
from jax.experimental.pallas import tpu as pltpu
from jax.sharding import PartitionSpec as P

NS_STEPS = 8
REFINE = 2
LANES = 2
PARTS = 4
F32 = jnp.float32
BF16 = jnp.bfloat16
MESH = pl.DeviceIdType.MESH


def mm(left, right):
    return lax.dot_general(left, right, (((1,), (0,)), ((), ())), preferred_element_type=F32)


def mm_nt(left, right):
    return lax.dot_general(left, right, (((1,), (1,)), ((), ())), preferred_element_type=F32)


def mm_tn(left, right):
    return lax.dot_general(left, right, (((0,), (0,)), ((), ())), preferred_element_type=F32)


def halves(value):
    high = value.astype(BF16)
    low = (value - high.astype(F32)).astype(BF16)
    return jnp.concatenate([high, low], axis=1)


def fold(wide):
    width = wide.shape[1] // 2
    return wide[:, :width] + wide[:, width:]


def twice(pair):
    return jnp.concatenate([pair, pair], axis=0)


def kernel(
    chain,
    gain_hbm, ridge_hbm, query_hbm, key_hbm, value_hbm, out_ref,
    gain_ref, ridge_ref,
    query_ref, key_ref, value_ref,
    keys, turned_keys, gram_parts, gram_all, cross_head, cross_all,
    gram_in, gram_out, gram_side, cross_in, cross_out, cross_mix, cross_half, cross_side,
    weights, start, solved, final,
    query_sem, key_sem, value_sem, gain_sem, ridge_sem,
    gram_send, gram_recv, side_send, side_recv,
    cross_send, cross_recv, half_send, half_recv, cside_send, cside_recv,
):
    heads, dim, tokens = turned_keys.shape
    sub, part = tokens // 2, tokens // PARTS
    pairs = heads // 2
    place = lax.axis_index("seq")
    row, lane = place // LANES, place % LANES
    partner = place + 1 - 2 * lane
    has_prev, has_next = row > 0, row < chain - 1
    gets_side = jnp.logical_or(lane == 1, has_prev)

    barrier = pltpu.get_barrier_semaphore()

    def greet(device):
        pl.semaphore_signal(barrier, inc=1, device_id={"seq": device}, device_id_type=MESH)

    greet(partner)

    @pl.when(has_prev)
    def _():
        greet(place - LANES)

    @pl.when(has_next)
    def _():
        greet(place + LANES)

    def pair_cols(p):
        return slice(2 * p * dim, 2 * (p + 1) * dim)

    def fetch(p, src, dst, sem):
        return pltpu.make_async_copy(src.at[:, pair_cols(p)], dst.at[:, pair_cols(p)], sem.at[p])

    gains = pltpu.make_async_copy(gain_hbm, gain_ref, gain_sem)
    ridges = pltpu.make_async_copy(ridge_hbm, ridge_ref, ridge_sem)
    fetch(0, key_hbm, key_ref, key_sem).start()
    gains.start()
    for p in range(1, pairs):
        fetch(p, key_hbm, key_ref, key_sem).start()
    ridges.start()
    values_in = pltpu.make_async_copy(value_hbm, value_ref, value_sem)
    queries_in = pltpu.make_async_copy(query_hbm, query_ref, query_sem)
    values_in.start()
    queries_in.start()

    i = lax.broadcasted_iota(jnp.int32, (dim, dim), 0)
    j = lax.broadcasted_iota(jnp.int32, (dim, dim), 1)
    eye = jnp.where(i == j, 1.0, 0.0).astype(F32)

    def copy(src, dst, send, recv, device):
        return pltpu.make_async_remote_copy(
            src_ref=src, dst_ref=dst, send_sem=send, recv_sem=recv,
            device_id={"seq": device}, device_id_type=MESH,
        )

    first_row = jnp.logical_not(has_prev)
    last_row = jnp.logical_and(has_prev, jnp.logical_not(has_next))
    middle = jnp.logical_and(has_prev, has_next)
    cuts = [dim // 4, dim // 2, 3 * dim // 4, dim + 8]
    quarters = [slice(a, b) for a, b in zip([0] + cuts[:-1], cuts)]
    halved = [slice(0, cuts[1]), slice(cuts[1], cuts[3])]
    spans = {(p, q): span for p in range(pairs) for q, span in enumerate(halved if p else quarters)}
    number = {piece: n for n, piece in enumerate(spans)}

    def pieces(p):
        return [q for k, q in spans if k == p]

    def gram_next(p, q):
        n = number[p, q]
        return copy(
            gram_out.at[p, spans[p, q]], gram_in.at[p, spans[p, q]],
            gram_send, gram_recv.at[n], place + LANES,
        )

    def gram_across(p, q, src):
        return copy(
            src.at[p, spans[p, q]], gram_side.at[p, spans[p, q]],
            side_send, side_recv.at[p], partner,
        )

    def side_of(p):
        return copy(gram_out.at[p], gram_side.at[p], side_send, side_recv.at[p], partner)

    def cross_next(p):
        return copy(cross_out.at[p], cross_in.at[p], cross_send, cross_recv.at[p], place + LANES)

    def cross_across(p, src):
        return copy(src.at[p], cross_side.at[p], cside_send, cside_recv.at[p], partner)

    def send_side(p):
        @pl.when(jnp.logical_and(first_row, lane == 0))
        def _():
            for q in pieces(p):
                gram_across(p, q, gram_out).start()

    def relay_gram(p):
        for q in pieces(p):
            gram_next(p, q).wait_recv()

            @pl.when(lane == 1)
            def _():
                gram_across(p, q, gram_in).start()

            gram_out[p, spans[p, q]] += gram_in[p, spans[p, q]]

            @pl.when(has_next)
            def _():
                gram_next(p, q).start()

            @pl.when(lane == 0)
            def _():
                gram_across(p, q, gram_out).start()

    def cross_swap(p):
        return copy(
            cross_all.at[2 * p + 1 - lane], cross_half.at[p],
            half_send, half_recv.at[p], partner,
        )

    def swap_cross(p):
        @pl.when(jnp.logical_not(jnp.logical_and(last_row, lane == 1)))
        def _():
            cross_swap(p).start()

    def relay_cross(p):
        @pl.when(jnp.logical_not(jnp.logical_and(last_row, lane == 0)))
        def _():
            cross_swap(p).wait_recv()

        @pl.when(has_prev)
        def _():
            cross_next(p).wait_recv()

            @pl.when(lane == 1)
            def _():
                cross_across(p, cross_in).start()

        mixed = cross_in[p] + cross_all[2 * p + lane]

        @pl.when(lane == 0)
        def _():
            cross_mix[p] = mixed
            cross_across(p, cross_mix).start()

        @pl.when(has_next)
        def _():
            cross_out[p] = mixed + cross_half[p]
            cross_next(p).start()

    gains.wait()
    for p in range(pairs):
        fetch(p, key_hbm, key_ref, key_sem).wait()
        for h in (2 * p, 2 * p + 1):
            raw = key_ref[:, h * dim : (h + 1) * dim].astype(F32)
            scaled = (raw * gain_ref[h]).astype(BF16)
            turned = scaled.T
            keys[p, :, (h - 2 * p) * dim : (h - 2 * p + 1) * dim] = scaled
            turned_keys[h] = turned
            gram_all[h] = mm(turned, scaled)
        upper, lower = gram_all[2 * p], gram_all[2 * p + 1]
        gram_out[p, :dim] = jnp.where(i <= j, upper, lower)
        diagonal = jnp.sum(jnp.where(i == j, lower, 0.0), axis=0, keepdims=True)
        gram_out[p, dim:] = jnp.broadcast_to(diagonal, (8, dim))
        if p == 0:
            pl.semaphore_wait(barrier, 1 + has_prev.astype(jnp.int32) + has_next.astype(jnp.int32))

        @pl.when(jnp.logical_and(first_row, has_next))
        def _():
            for q in pieces(p):
                gram_next(p, q).start()

        if p == 0:
            send_side(p)

    values_in.wait()
    for p in range(pairs):
        for h in (2 * p, 2 * p + 1):
            values = value_ref[:, h * dim : (h + 1) * dim]
            first = mm(turned_keys[h, :, :sub], values[:sub])
            total = first + mm(turned_keys[h, :, sub:], values[sub:])
            cross_head[h] = first
            cross_all[h] = total
        if p < 2:
            swap_cross(p)
        else:
            @pl.when(jnp.logical_not(middle))
            def _():
                swap_cross(p)
    for p in range(1, pairs):
        send_side(p)

    @pl.when(first_row)
    def _():
        gram_in[...] = jnp.zeros_like(gram_in)
        cross_in[...] = jnp.zeros_like(cross_in)

    @pl.when(jnp.logical_and(last_row, lane == 0))
    def _():
        cross_half[...] = jnp.zeros_like(cross_half)

    @pl.when(jnp.logical_not(gets_side))
    def _():
        gram_side[...] = jnp.zeros_like(gram_side)
        cross_side[...] = jnp.zeros_like(cross_side)

    ridges.wait()
    queries_in.wait()

    second_row = jnp.logical_and(middle, row == 1)

    @pl.when(second_row)
    def _():
        relay_gram(0)

    weights[:, :, :, :part, dim:] = jnp.zeros((2, 2, PARTS, part, dim), BF16)
    for h in range(heads):
        total = None
        for s in range(PARTS - 1):
            rows = slice(s * part, (s + 1) * part)
            cols = slice(h % 2 * dim, (h % 2 + 1) * dim)
            gram = mm(turned_keys[h, :, rows], keys[h // 2, rows, cols])
            total = gram if total is None else total + gram
            gram_parts[h, s * dim : (s + 1) * dim] = halves(total)

    @pl.when(jnp.logical_and(middle, row > 1))
    def _():
        relay_gram(0)

    @pl.when(middle)
    def _():
        for p in range(1, pairs):
            relay_gram(p)
            if p < pairs - 1:
                cross_swap(p + 1).start()

    @pl.when(last_row)
    def _():
        for p in range(min(2, pairs)):
            relay_gram(p)

    def arrive(p):
        @pl.when(gets_side)
        def _():
            side_of(p).wait_recv()

    def precondition(p, result):
        packed = gram_in[p] + gram_side[p]
        square = packed[:dim]
        turned = square.T
        upper = jnp.where(i <= j, square, turned)
        lower = jnp.where(i > j, square, jnp.where(i < j, turned, packed[dim : dim + 1]))
        state = []
        for h, prior in ((2 * p, upper), (2 * p + 1, lower)):
            plain = ridge_ref[h] * eye + prior
            end = plain + gram_all[h]
            gram_all[h] = plain
            total = jnp.sum(jnp.sum(end * end, axis=1, keepdims=True), axis=0, keepdims=True)
            inverse = 1.0 / jnp.sqrt(total)
            rest = eye - end * inverse
            split = halves(rest)
            both = jnp.concatenate([fold(mm(split, twice(split))), eye + rest], axis=0)
            state.append((both, inverse))
        yield
        for step in range(NS_STEPS - 2):
            for k in range(2):
                both, inverse = state[k]
                split = halves(both)
                product = fold(mm(split, twice(split[:dim])))
                both = jnp.concatenate([product[:dim], both[dim:] + product[dim:]], axis=0)
                state[k] = (both, inverse)
            yield
        for both, inverse in state:
            split = halves(both)
            approx = both[dim:] + fold(mm(split[dim:], twice(split[:dim])))
            result.append(halves(approx * inverse))
        yield

    def causal(size):
        t = lax.broadcasted_iota(jnp.int32, (size, size), 0)
        u = lax.broadcasted_iota(jnp.int32, (size, size), 1)
        return t >= u

    def solve(p, preconds):
        slot = p % 2
        blank = jnp.zeros((dim, dim), BF16)
        both = jnp.concatenate([
            jnp.concatenate([preconds[0][:, :dim], blank], axis=1),
            jnp.concatenate([blank, preconds[1][:, :dim]], axis=1),
        ], axis=0)
        shifted = (-mm(keys[p], both)).astype(BF16)
        scores, current = {}, {}

        def prepare(k):
            h = 2 * p + k
            precond = preconds[k]
            start[slot, k] = fold(mm(query_ref[:, h * dim : (h + 1) * dim], precond))
            stack = jnp.concatenate([halves(gram_all[h]), gram_parts[h]], axis=0)
            product = fold(mm(stack, twice(precond)))
            rest = eye - product[:dim]
            for s in range(PARTS):
                left = rest - product[s * dim : (s + 1) * dim] if s else rest
                weights[slot, k, s, :part, :dim] = shifted[s * part : (s + 1) * part, k * dim : (k + 1) * dim]
                weights[slot, k, s, part:] = halves(left)
                current[k, s] = start[slot, k, s * part : (s + 1) * part].astype(BF16)

        def score(k):
            for s in range(PARTS):
                product = mm(current[k, s], turned_keys[2 * p + k, :, s * part : (s + 1) * part])
                scores[k, s] = jnp.where(causal(part), product, 0.0).astype(BF16)

        def update(k, last):
            for s in range(PARTS):
                rows = slice(s * part, (s + 1) * part)
                both = jnp.concatenate([scores[k, s], current[k, s]], axis=1)
                value = start[slot, k, rows] + fold(mm(both, weights[slot, k, s]))
                if last:
                    solved[2 * p + k, rows] = halves(value)
                else:
                    current[k, s] = value.astype(BF16)

        prepare(0)
        yield
        prepare(1)
        score(0)
        yield
        for repeat in range(REFINE):
            last = repeat == REFINE - 1
            update(0, last)
            score(1)
            yield
            update(1, last)
            if not last:
                score(0)
            yield

    def weave(*streams):
        streams = list(streams)
        while streams:
            streams = [stream for stream in streams if next(stream, 0) is None]

    rows = jnp.minimum(row, 2)
    roles = (
        (first_row, (0, 0, 0, 0)),
        (jnp.logical_and(middle, rows == 1), (0, 0, 0, 1)),
        (jnp.logical_and(middle, rows == 2), (0, 1, 1, 2)),
        (last_row, (1, 2, 2, 3)),
    )
    end = pairs

    def relay_at(slot):
        for role, slots in roles:
            units = [p for p in range(pairs) if min(slots[min(p, 3)], end) == slot]
            if units:
                @pl.when(role)
                def _():
                    for p in units:
                        relay_cross(p)

    def cross_arrive(p):
        @pl.when(gets_side)
        def _():
            cross_across(p, cross_in).wait_recv()

    def read(p):
        for k in range(2):
            h = 2 * p + k
            cols = pl.ds(pl.multiple_of(h * dim, dim), dim)
            own = cross_in[p] + jnp.where(lane == 1, cross_half[p], 0.0)
            prior = jnp.where(lane == k, own, cross_side[p])
            for s in range(2):
                rows = slice(s * sub, (s + 1) * sub)
                values = value_ref[rows, cols]
                final[k, s, :sub] = jnp.concatenate([values, jnp.zeros_like(values)], axis=1)
                matrix = prior if s == 0 else prior + cross_head[h]
                final[k, s, sub:] = twice(halves(matrix))
                split = solved[h, rows]
                scores = mm(split[:, :dim], turned_keys[h, :, rows])
                scores = jnp.where(causal(sub), scores, 0.0).astype(BF16)
                total = mm(jnp.concatenate([scores, split], axis=1), final[k, s])
                out_ref[rows, cols] = fold(total).astype(BF16)
                yield

    early = min(1, pairs - 1)

    arrive(0)

    @pl.when(last_row)
    def _():
        for p in range(2, min(3, pairs)):
            relay_gram(p)

    preconds = []
    weave(precondition(0, preconds))

    @pl.when(last_row)
    def _():
        for p in range(3, pairs):
            relay_gram(p)

    relay_at(0)
    for p in range(pairs):
        later = []
        streams = [solve(p, preconds)]
        if p + 1 < pairs:
            arrive(p + 1)
            streams.append(precondition(p + 1, later))
        elif early:
            cross_arrive(0)
            streams.append(read(0))
        weave(*streams)
        relay_at(p + 1)
        preconds = later

    def read_pair(p, carry):
        cross_arrive(p)
        for _ in read(p):
            pass
        return carry

    lax.fori_loop(early, pairs, read_pair, 0)

    @pl.when(jnp.logical_not(jnp.logical_and(last_row, lane == 1)))
    def _():
        copy(cross_out, cross_half, half_send, half_recv.at[0], partner).wait_send()

    @pl.when(has_next)
    def _():
        copy(gram_out, gram_in, gram_send, gram_recv.at[0], place + LANES).wait_send()
        copy(cross_out, cross_in, cross_send, cross_recv.at[0], place + LANES).wait_send()

    @pl.when(jnp.logical_or(lane == 0, has_prev))
    def _():
        copy(gram_out, gram_side, side_send, side_recv.at[0], partner).wait_send()
        copy(cross_out, cross_side, cside_send, cside_recv.at[0], partner).wait_send()


def solution(mesh):
    chain = mesh.shape["seq"] // LANES

    def body(query_rows, key_rows, value_rows, key_gain, regularizer):
        heads = key_gain.shape[0]
        tokens, width = query_rows.shape
        dim = width // heads
        sub, pairs = tokens // 2, heads // 2
        vmem = pl.BlockSpec(memory_space=pltpu.VMEM)
        hbm = pl.BlockSpec(memory_space=pl.ANY)
        rows = pltpu.VMEM((tokens, width), BF16)
        square = pltpu.VMEM((heads, dim, dim), F32)
        packed = pltpu.VMEM((pairs, dim + 8, dim), F32)
        crosses = pltpu.VMEM((pairs, dim, dim), F32)
        single = pltpu.SemaphoreType.DMA
        return pl.pallas_call(
            functools.partial(kernel, chain),
            out_shape=pltpu.VMEM((tokens, width), BF16),
            in_specs=[hbm] * 5,
            out_specs=vmem,
            scratch_shapes=[
                pltpu.SMEM((heads,), F32), pltpu.SMEM((heads,), F32),
                rows, rows, rows,
                pltpu.VMEM((pairs, tokens, 2 * dim), BF16),
                pltpu.VMEM((heads, dim, tokens), BF16),
                pltpu.VMEM((heads, (PARTS - 1) * dim, 2 * dim), BF16),
                square, square, square,
                packed, packed, packed,
                crosses, crosses, crosses, crosses, crosses,
                pltpu.VMEM((2, 2, PARTS, tokens // PARTS + dim, 2 * dim), BF16),
                pltpu.VMEM((2, 2, tokens, dim), F32),
                pltpu.VMEM((heads, tokens, 2 * dim), BF16),
                pltpu.VMEM((2, 2, sub + 2 * dim, 2 * dim), BF16),
            ]
            + [single, pltpu.SemaphoreType.DMA((pairs,))] + [single] * 3
            + [single, pltpu.SemaphoreType.DMA((2 * pairs + 2,))]
            + [single, pltpu.SemaphoreType.DMA((pairs,))] * 4,
            compiler_params=pltpu.CompilerParams(collective_id=0, has_side_effects=True),
            name="mesa_prefill",
        )(key_gain, regularizer, query_rows, key_rows, value_rows)

    placed = (P("seq", "head"), P("seq", "head"), P("seq", "head"), P("head"), P("head"))
    return jax.shard_map(
        body, mesh=mesh, in_specs=placed, out_specs=P("seq", "head"), check_vma=False
    )
```
